512 devices in a mesh: groups: 2 (over y), ep: 32 (over z), tp: 4 (over x), dp: 2 (over core).
Axes of the slice: x: 4, y: 2, z: 32, core: 2. Of those that a mesh axis runs over, the one named last changes fastest.
The devices are a block of a 4x8x32 slice.
Arguments:
- tokens: bfloat16 [4096, 5120], P(('groups', 'ep', 'tp', 'dp')), parts along dimension 0, may hold values from -6 to 6
- route_weights: float32 [4096, 8], P(('groups', 'ep', 'tp', 'dp')), parts along dimension 0, may hold values from 0.1 to 1
- expert_ids: int32 [4096, 8], P(('groups', 'ep', 'tp', 'dp')), parts along dimension 0, may hold values from 0 to 31, all different within a row; in each aligned block of 8 rows (0 to 7, 8 to 15, ...) at most 4 rows name the same one
- gate_weight: bfloat16 [32, 5120, 1024], P('ep', None, ('tp', 'dp')), may hold values from -0.078125 to 0.078125
- up_weight: bfloat16 [32, 5120, 1024], P('ep', None, ('tp', 'dp')), may hold values from -0.078125 to 0.078125
- down_weight: bfloat16 [32, 1024, 5120], P('ep', None, ('tp', 'dp')), may hold values from -0.1875 to 0.1875
Outputs:
- combined: bfloat16 [4096, 5120], P(('groups', 'ep', 'tp', 'dp')), parts along dimension 0
The draws below stay inside these ranges and needn't reach their ends.
There are 2 independent parts, one for each index of `groups`. The reference program is written for one: setup_inputs(seed, part) draws one part's arguments, and reference() takes and returns one part's arrays. A program takes and returns all parts, laid end to end along the dimension named above; an argument that names none is the same for every part. Nothing has to cross between parts.
Inputs may be any that keep to these rules, and one draw needn't show every extreme that they name: `expert_ids`: each row names 8 different experts. Among the 8 rows of one device no expert is named more than 4 times, and in every draw some device's rows name some expert exactly 4 times.
All inputs are finite; a program needn't handle non-finite values.
Results may differ from the reference program's by a relative error of at most 0.0057.
Values may be sent and summed in bfloat16 or wider, within the bound.
A program may use at most 64 MiB of HBM per device.

```python
import math
import jax
import jax.numpy as jnp
import numpy as np
from jax import lax

D = 5120
FF = 1024
EXPERTS = 32
TOP = 8
TOK_DEV = 8
CAP = 4
TOKENS = 2048
N_EP = 32
N_TP = 4
N_DP = 2


def block_levels(own_key, dims, shards, low, top_value):
    gain = 1.0
    for dim, shards_of in shards:
        heights = jax.random.uniform(jax.random.fold_in(jax.random.fold_in(own_key, 6), dim), (shards_of,), jnp.float32, low / len(shards), top_value / len(shards))
        gain = gain * jnp.repeat(jnp.exp(heights), dims[dim] // shards_of).reshape((-1,) + (1,) * (len(dims) - 1 - dim))
    return gain


def deal_out(key, own, number, rows, count, top, most, lean):
    sequence = jax.random.permutation(key, count)
    heavy_load, usual = portions_of(count, rows * top, most, lean, True), portions_of(count, rows * top, most, lean, False)
    places = jnp.arange(count)

    def named(tallies, turn):
        used = int((tallies > 0).sum())
        fixed = max(1, used // 4)
        passed = fixed + (places - fixed + turn * (used - fixed)) % max(1, count - fixed)
        return jnp.zeros((count,), jnp.int32).at[sequence[jnp.where(places < fixed, places, passed)]].set(jnp.asarray(tallies, jnp.int32))

    tallies = jnp.where(number % 4 == 0, named(heavy_load, number // 4), named(usual, number - number // 4 - 1))
    mixed = jax.random.permutation(jax.random.fold_in(own, 3), count)
    donor, sink = mixed[0:count // 2 * 2:2], mixed[1:count // 2 * 2:2]
    slack = jnp.minimum(tallies[donor] - 1, most - tallies[sink]) // 2
    slack = jnp.where((donor == sequence[0]) | (sink == sequence[0]) | (tallies[sink] == 0), 0, jnp.maximum(slack, 0))
    passed = jax.random.randint(jax.random.fold_in(own, 4), (count // 2,), 0, 1 << 20) % (slack + 1)
    tallies = tallies.at[donor].add(-passed).at[sink].add(passed)
    members = jnp.searchsorted(jnp.cumsum(tallies), jnp.arange(rows * top), side="right").astype(jnp.int32)
    grid = members.reshape(top, rows).T
    grid = grid[jax.random.permutation(jax.random.fold_in(own, 1), rows)]
    turn = jax.random.randint(jax.random.fold_in(own, 2), (rows, 1), 0, top)
    return jnp.take_along_axis(grid, (jnp.arange(top)[None, :] + turn) % top, axis=1)


def portions_of(number_of, total, most, lean, full):
    weights = [(1 << 20) // math.isqrt(rank ** lean) + 1 for rank in range(1, number_of + 1)]
    largest = most if full else min(most, max(-(-total // number_of), total * weights[0] // sum(weights)))
    least = 1 if total - largest >= number_of - 1 else 0
    given, spare = [largest] + [least] * (number_of - 1), total - largest - least * (number_of - 1)
    while spare > 0:
        candidates = [i for i in range(1, number_of) if given[i] < largest] or [i for i in range(1, number_of) if given[i] < most]
        mass, budget = sum([weights[i] for i in candidates]), spare
        for i in candidates:
            extra = min(most - given[i], max(1, budget * weights[i] // mass), spare)
            given[i] = given[i] + extra
            spare = spare - extra
    return np.array(given)


def normal_values(stream_key, dims, deviation, limit, shards=(), held_as=jnp.bfloat16):
    array = jax.random.normal(stream_key, dims, jnp.float32) * deviation
    if len(shards) > 0:
        array = block_levels(stream_key, dims, shards, -0.22, 0.18) * array
    return jnp.clip(array, min=-limit, max=limit).astype(held_as)


def setup_inputs(seed: int = 0, part: int = 0) -> dict:
    streams_of = jax.random.split(jax.random.key(seed), 7)
    own_keys = jax.random.split(jax.random.fold_in(streams_of[6], part), 7)
    tokens = normal_values(own_keys[0], (TOKENS, D), 1.0, 6.0, ((0, 256),))
    route_weights = jnp.clip(jnp.exp(math.log(1.0) - 2.3025851 * jax.random.uniform(own_keys[1], (TOKENS, TOP), jnp.float32) ** block_levels(own_keys[1], (TOKENS, TOP), ((0, 256),), -0.2, 0.2)), 0.1, 1.0)
    expert_ids_keys = jax.random.split(jax.random.fold_in(own_keys[2], 1), TOKENS // TOK_DEV)
    expert_ids_turns = jax.random.permutation(jax.random.fold_in(own_keys[2], 3), TOKENS // TOK_DEV)
    expert_ids = jax.vmap(lambda own, number: deal_out(jax.random.fold_in(own_keys[2], 2), own, number, TOK_DEV, EXPERTS, TOP, CAP, 2))(expert_ids_keys, expert_ids_turns).reshape((TOKENS, TOP))
    gate_weight = normal_values(streams_of[3], (EXPERTS, D, FF), D ** -0.5, 0.078125, ((0, 32), (2, 8)))
    up_weight = normal_values(streams_of[4], (EXPERTS, D, FF), D ** -0.5, 0.078125, ((0, 32), (2, 8)))
    down_weight = normal_values(streams_of[5], (EXPERTS, FF, D), FF ** -0.5, 0.1875, ((0, 32), (2, 8)))
    return dict(tokens=tokens, route_weights=route_weights, expert_ids=expert_ids, gate_weight=gate_weight, up_weight=up_weight, down_weight=down_weight)


def reference(tokens, route_weights, expert_ids, gate_weight, up_weight, down_weight):
    devices = N_EP * N_TP * N_DP
    blocks = expert_ids.reshape(devices, TOK_DEV * TOP)
    onehot = (blocks[:, :, None] == jnp.arange(EXPERTS, dtype=jnp.int32)[None, None, :]).astype(jnp.int32)
    slots = jnp.sum(onehot * jnp.cumsum(onehot, axis=1), axis=2) - 1
    device_ids = jnp.arange(devices, dtype=jnp.int32)[:, None]
    position = (device_ids * CAP + slots).reshape(-1).astype(jnp.int32)
    flat_ids = expert_ids.reshape(-1).astype(jnp.int32)
    owner = (jnp.arange(TOKENS * TOP, dtype=jnp.int32) // TOP).astype(jnp.int32)
    span = devices * CAP

    def one_expert(expert):
        index = jnp.where(flat_ids == expert, position, span).astype(jnp.int32)
        table = jnp.full((span,), TOKENS, jnp.int32).at[index].set(owner, mode="drop")
        rows = jnp.take(tokens, table, axis=0, mode="fill", fill_value=0)
        gate = jnp.dot(rows, gate_weight[expert], preferred_element_type=jnp.float32)
        up = jnp.dot(rows, up_weight[expert], preferred_element_type=jnp.float32)
        hidden = (jax.nn.silu(gate) * up).astype(jnp.bfloat16)
        return jnp.dot(hidden, down_weight[expert], preferred_element_type=jnp.float32).astype(jnp.bfloat16)

    outputs = lax.map(one_expert, jnp.arange(EXPERTS, dtype=jnp.int32))
    flat_out = outputs.reshape(EXPERTS * span, D)
    picked_index = (flat_ids * span + position).reshape(TOKENS, TOP).astype(jnp.int32)
    total = jnp.zeros((TOKENS, D), jnp.float32)
    for route in range(TOP):
        chosen = jnp.take(flat_out, picked_index[:, route], axis=0).astype(jnp.float32)
        total = total + route_weights[:, route:route + 1] * chosen
    return total.astype(jnp.bfloat16)
```

```python
import jax
import jax.numpy as jnp
from jax import lax
from jax.sharding import PartitionSpec as P

CAP = 4
META = 128


def pieces(w):
    hi = w.astype(jnp.bfloat16)
    rest = w - hi.astype(jnp.float32)
    mid = rest.astype(jnp.bfloat16)
    low = (rest - mid.astype(jnp.float32)).astype(jnp.bfloat16)
    return jnp.concatenate([hi, mid, low], axis=-1)


def per_device(tokens, route_weights, expert_ids, gate_weight, up_weight, down_weight):
    n_ep = lax.axis_size("ep")
    rows, width = tokens.shape
    named = expert_ids[:, :, None] == jnp.arange(n_ep, dtype=jnp.int32)[None, None, :]
    dense = jnp.sum(jnp.where(named, route_weights[:, :, None], 0.0), axis=1)
    eye = jnp.eye(rows, dtype=jnp.bfloat16)
    meta = jnp.concatenate([pieces(dense), eye], axis=1)
    meta = jnp.pad(meta, ((0, 0), (0, META - meta.shape[1])))
    sent = jnp.concatenate([tokens, meta], axis=1)
    got = lax.all_gather(sent, "ep", axis=0)
    me = lax.axis_index("ep")

    def weight_of(block):
        m = block[..., width:].astype(jnp.float32)
        part = [lax.dynamic_slice_in_dim(m, me + j * n_ep, 1, axis=-1) for j in range(3)]
        return (part[0] + part[1] + part[2])[..., 0]

    mask = weight_of(got) > 0
    slot = jnp.cumsum(mask.astype(jnp.int32), axis=1) - 1
    pick = mask[:, None, :] & (slot[:, None, :] == jnp.arange(CAP)[None, :, None])
    sel = jnp.einsum("bst,btd->bsd", pick.astype(jnp.bfloat16), got, preferred_element_type=jnp.bfloat16)
    piece = lax.all_gather(sel, ("tp", "dp"), axis=0)
    x = piece[..., :width]
    gate = jnp.einsum("gbsd,df->gbsf", x, gate_weight[0], preferred_element_type=jnp.float32)
    up = jnp.einsum("gbsd,df->gbsf", x, up_weight[0], preferred_element_type=jnp.float32)
    hidden = (jax.nn.silu(gate) * up).astype(jnp.bfloat16)
    hidden = lax.all_gather(hidden, ("tp", "dp"), axis=3, tiled=True)
    out = jnp.einsum("gbsf,fd->gbsd", hidden, down_weight[0], preferred_element_type=jnp.float32).astype(jnp.bfloat16)
    code = piece[..., width + 3 * n_ep : width + 3 * n_ep + rows]
    w = weight_of(piece)
    w_tok = jnp.sum(code.astype(jnp.float32) * w[..., None], axis=2)
    back = jnp.einsum("gbst,gbsd->bgtd", code, out, preferred_element_type=jnp.float32)
    back = (back * jnp.swapaxes(w_tok, 0, 1)[..., None]).astype(jnp.bfloat16)
    flat = back.reshape(n_ep * back.shape[1] * rows, back.shape[3])
    summed = lax.psum_scatter(flat, "ep", scatter_dimension=0, tiled=True)
    summed = summed.reshape(back.shape[1], rows, back.shape[3])
    mine = lax.all_to_all(summed, ("tp", "dp"), split_axis=0, concat_axis=2, tiled=True)
    return mine[0]


def solution(mesh):
    tok = P(("groups", "ep", "tp", "dp"), None)
    wgt = P("ep", None, ("tp", "dp"))
    return jax.shard_map(
        per_device,
        mesh=mesh,
        in_specs=(tok, tok, tok, wgt, wgt, wgt),
        out_specs=tok,
        check_vma=False,
    )
```
